32 devices in a mesh: rows: 16 (over z, x, core), inner: 2 (over y).
Axes of the slice: x: 2, y: 2, z: 4, core: 2. Of those that a mesh axis runs over, the one named last changes fastest.
Arguments:
- blocks: bfloat16 [16, 16, 256, 256], P('rows'), may hold values from -0.375 to 0.375
- columns: int32 [16, 16], replicated, may hold values from -1 to 15, as said below
Outputs:
- purified: float32 [16, 16, 256, 256], P('rows', None, 'inner')
The draws below stay inside these ranges and needn't reach their ends.
Inputs may be any that keep to these rules, and one draw needn't show every extreme that they name: Each entry of row i that is not -1 is (i + d) mod 16 for an offset d with -16 <= 2 * d < 16; the entries of a row are distinct and stand before its -1 entries; every row lists its diagonal block; some row lists 16 columns.
All inputs are finite; a program needn't handle non-finite values.
Results may differ from the reference program's by a relative error of at most 0.0055.
Values may be sent and summed in bfloat16 or wider, within the bound.
A program may use at most 128 MiB of HBM per device.

```python
import jax
import jax.numpy as jnp
from jax import lax

BS = 256
BAND = 16
NB = 16
N_INNER = 2


def draw_columns(key, part):
    half_band = BAND // 2
    first_key, second_key, third_key = jax.random.split(jax.random.fold_in(key, 11), 3)
    density = jax.random.randint(first_key, (NB, 1), 24, 96)
    rolls = jax.random.randint(second_key, (NB, BAND), 0, 64)
    slot_ids = jnp.arange(BAND, dtype=jnp.int32)
    distance = 3 * jnp.abs(slot_ids - half_band)
    live_slots = rolls < density - distance[None, :]
    full_row = jax.random.randint(third_key, (), 0, NB)
    row_ids = jnp.arange(NB, dtype=jnp.int32)
    live_slots = live_slots | (slot_ids[None, :] == half_band) | (row_ids[:, None] == full_row)
    sort_keys = jnp.where(live_slots, slot_ids[None, :], slot_ids[None, :] + BAND)
    order = jnp.argsort(sort_keys, axis=1, stable=True).astype(jnp.int32)
    live_sorted = jnp.take_along_axis(live_slots, order, axis=1)
    block_cols = (row_ids[:, None] + order - half_band) % NB
    return jnp.where(live_sorted, block_cols, -1).astype(jnp.int32)


def block_levels(key, dims, shards, least, largest):
    factor_of, own = 1.0, jax.random.fold_in(key, 6)
    for axis_at, shards_of in shards:
        heights = jnp.exp(jax.random.uniform(jax.random.fold_in(own, axis_at), (shards_of,), jnp.float32, least / len(shards), largest / len(shards)))
        factor_of = factor_of * jnp.repeat(heights, dims[axis_at] // shards_of).reshape([-1 if axis == axis_at else 1 for axis in range(len(dims))])
    return factor_of


def gaussian(stream_key, shape, width, reach, cuts=(), held_as=jnp.bfloat16):
    entries = width * jax.random.normal(stream_key, shape, jnp.float32)
    if cuts:
        entries = entries * block_levels(stream_key, shape, cuts, -0.22, 0.18)
    return jnp.clip(entries, -reach, reach).astype(held_as)


def setup_inputs(seed: int = 0) -> dict:
    arg_keys = jax.random.split(jax.random.key(seed), 3)
    blocks = gaussian(arg_keys[0], (NB, BAND, BS, BS), BS ** -0.5, 0.375, ((0, 16),))
    columns = draw_columns(jax.random.fold_in(arg_keys[2], 71), 0)
    return dict(blocks=blocks, columns=columns)


def live_table(columns):
    nrows, band_width = columns.shape
    half_band = band_width // 2
    row_ids = jnp.arange(nrows, dtype=jnp.int32)
    target = (row_ids[:, None] + jnp.arange(band_width, dtype=jnp.int32)[None, :] - half_band) % nrows
    return jnp.any(columns[:, None, :] == target[:, :, None], axis=2)


def slot_shift(piece, delta):
    band_width = piece.shape[1]
    if delta >= 0:
        return jnp.concatenate([piece[:, delta:], jnp.zeros_like(piece[:, :delta])], axis=1)
    return jnp.concatenate([jnp.zeros_like(piece[:, :(-delta)]), piece[:, :band_width + delta]], axis=1)


def band_product(left_all, right_all):
    nrows, band_width, block_size, _ = left_all.shape
    half_band = band_width // 2
    slab_width = block_size // N_INNER

    def one_row(row_index):
        row_ids = (row_index + jnp.arange(band_width, dtype=jnp.int32) - half_band) % nrows
        right_rows = right_all[row_ids]
        left_rows = left_all[row_index]
        totals = jnp.zeros((N_INNER, band_width, block_size, block_size), jnp.float32)
        for offset in range(band_width):
            shifted = slot_shift(right_rows[offset][None], half_band - offset)[0]
            left_slab = left_rows[offset].astype(jnp.float32).reshape(block_size, N_INNER, slab_width)
            right_slab = shifted.astype(jnp.float32).reshape(band_width, N_INNER, slab_width, block_size)
            totals = totals + jnp.einsum("mcq,scqn->csmn", left_slab, right_slab)
        rounded = lax.optimization_barrier(totals.astype(jnp.bfloat16))
        return jnp.sum(rounded.astype(jnp.float32), axis=0)

    return lax.map(one_row, jnp.arange(nrows, dtype=jnp.int32))


def reference(blocks, columns):
    live_slots = live_table(columns)[:, :, None, None]
    masked = jnp.where(live_slots, blocks, jnp.zeros_like(blocks))
    square = jnp.where(live_slots, band_product(masked, masked), jnp.float32(0.0)).astype(jnp.bfloat16)
    cubed = jnp.where(live_slots, band_product(masked, square), jnp.float32(0.0))
    return 3.0 * square.astype(jnp.float32) - 2.0 * cubed
```

```python
import functools

import jax
import jax.numpy as jnp
from jax import lax
from jax.experimental import pallas as pl
from jax.experimental.pallas import tpu as pltpu
from jax.sharding import PartitionSpec as P

MESH = pl.DeviceIdType.MESH

def grid_kernel(own, lane_live, out, other, panels, acc, pure, final,
                left_send, left_recv, pass_send, pass_recv, panel_send, panel_recv, end_send, end_recv):
    half, slots, block, _ = own.shape
    slab = block // 2
    width = slots * slab
    rank, y = lax.axis_index("rows"), lax.axis_index("inner")
    rows = lax.axis_size("rows")
    core, x, z = rank % 2, (rank // 2) % 2, rank // 4
    upper, low = z // 2, z % 2
    parity = (upper + core) % 2
    to_core, to_x, to_z = 1 - 2 * core, 1 - 2 * x, 1 - 2 * low
    far_rank = lax.rem(rank + rows // 2, rows)
    at_far = {"rows": far_rank, "inner": y}
    at_y = {"rows": rank, "inner": 1 - y}
    at_far_y = {"rows": far_rank, "inner": 1 - y}
    at_z = {"rows": rank + 4 * to_z, "inner": y}
    at_x = {"rows": rank + 2 * to_x, "inner": y}
    at_core = {"rows": rank + to_core, "inner": y}
    everyone = (at_far, at_y, at_far_y, at_z, at_x, at_core)

    barrier = pltpu.get_barrier_semaphore()
    for device in everyone:
        pl.semaphore_signal(barrier, inc=1, device_id=device, device_id_type=MESH)

    here = pl.ds(pl.multiple_of(y * slab, slab), slab)
    there = pl.ds(pl.multiple_of((1 - y) * slab, slab), slab)
    sent = []

    def remote(source, target, send_sem, recv_sem, device):
        return pltpu.make_async_remote_copy(
            src_ref=source, dst_ref=target, send_sem=send_sem, recv_sem=recv_sem, device_id=device, device_id_type=MESH
        )

    def go(copy):
        copy.start()
        sent.append(copy)

    pieces = 4
    step = slots // pieces

    def left_piece(ref, number, which, side):
        if number == 0:
            return ref.at[which, :, :, side]
        return ref.at[which, (number - 1) * step : number * step, :, side]

    def send_left(number):
        which = 1 - parity if number == 0 else parity
        go(remote(left_piece(own, number, which, here), left_piece(other, number, which, here),
                  left_send.at[number], left_recv.at[number], at_far))

    def pass_left(number):
        which = parity if number == 0 else 1 - parity
        mine = left_piece(other, number, which, here)
        remote(mine, mine, left_send.at[number], left_recv.at[number], at_far).wait_recv()
        go(remote(mine, mine, pass_send.at[number], pass_recv.at[number], at_y))

    def end_left(number):
        which = parity if number == 0 else 1 - parity
        theirs = left_piece(other, number, which, there)
        remote(theirs, theirs, pass_send.at[number], pass_recv.at[number], at_y).wait_recv()

    def send_panel(product, source, target, send_at, device):
        go(remote(panels.at[product, source], panels.at[product, target],
                  panel_send.at[product, send_at], panel_recv.at[product, target], device))

    def take(product, source):
        ref = panels.at[product, source]
        remote(ref, ref, panel_send.at[product, 0], panel_recv.at[product, source], at_core).wait_recv()

    def share(product, source):
        send_panel(product, source, 8 + source, 8 + source, at_core)

    def spread(product, row):
        send_panel(product, row, 2 + row, row, at_z)
        send_panel(product, row, 4 + row, 2 + row, at_x)
        share(product, row)

    def mac(product, source, row, left):
        chip_core, chip, far = source // 8, (source // 2) % 4, source % 2
        delta = 4 * (to_z * (chip % 2) + 2 * far - 2 * row) + 2 * to_x * (chip // 2) + to_core * chip_core
        slot = (delta + 8 + 2 * rows) % rows
        shift = (slot + chip_core * (1 - 2 * parity)) // 2
        block_left = left[slot % 2, slot // 2]
        tile = 2 * slab
        for part in range(width // tile):
            lanes = pl.ds(pl.multiple_of(shift * slab + part * tile, slab), tile)
            acc[row, :, lanes] += jnp.dot(
                block_left, panels[product, source, :, part * tile : (part + 1) * tile],
                preferred_element_type=jnp.float32,
            )

    middle = slice(slots // 2 * slab, slots // 2 * slab + width)

    def masked_total(row):
        return jnp.where(lane_live[row : row + 1, :] > 0, acc[row, :, middle], 0.0)

    acc[...] = jnp.zeros_like(acc)
    for u in range(slots):
        panels[0, 0, :, u * slab : (u + 1) * slab] = own[parity, u, :, here]
    pl.semaphore_wait(barrier, len(everyone))

    send_left(0)
    spread(0, 0)
    for number in range(1, pieces + 1):
        send_left(number)

    def own_macs(sources):
        first, gap, count = sources

        def body(n, carry):
            mac(0, first + gap * n, 0, own)
            return carry

        lax.fori_loop(0, count, body, 0)

    own_macs((0, 1, 1))
    take(0, 2)
    send_panel(0, 2, 6, 4, at_x)
    share(0, 2)
    take(0, 4)
    share(0, 4)
    pass_left(0)
    for u in range(slots):
        panels[0, 1, :, u * slab : (u + 1) * slab] = other[parity, u, :, here]
    spread(0, 1)


    own_macs((1, 1, 2))
    own_macs((4, 1, 1))
    pass_left(1)
    take(0, 6)
    share(0, 6)
    take(0, 8)
    take(0, 10)
    take(0, 12)
    own_macs((6, 2, 4))
    pass_left(2)
    take(0, 3)
    send_panel(0, 3, 7, 5, at_x)
    share(0, 3)
    pass_left(3)
    take(0, 5)
    share(0, 5)
    take(0, 9)
    take(0, 14)
    own_macs((3, 2, 2))
    own_macs((9, 5, 2))
    pass_left(4)
    take(0, 11)
    take(0, 13)
    own_macs((11, 2, 2))
    take(0, 7)
    share(0, 7)
    own_macs((7, 8, 1))
    take(0, 15)
    own_macs((15, 1, 1))
    panels[1, 0] = masked_total(0).astype(panels.dtype)
    spread(1, 0)
    acc[0] = jnp.zeros_like(acc[0])

    for number in range(pieces + 1):
        end_left(number)

    def second_row(source, carry):
        mac(0, source, 1, other)
        return carry

    lax.fori_loop(0, rows, second_row, 0)
    panels[1, 1] = masked_total(1).astype(panels.dtype)
    spread(1, 1)
    acc[1] = jnp.zeros_like(acc[1])

    def pair_macs(first, gap, count):
        def body(n, carry):
            mac(1, first + gap * n, 0, own)
            mac(1, first + gap * n, 1, other)
            return carry

        lax.fori_loop(0, count, body, 0)

    pair_macs(0, 1, 2)
    take(1, 2)
    send_panel(1, 2, 6, 4, at_x)
    share(1, 2)
    take(1, 4)
    share(1, 4)
    take(1, 8)
    take(1, 9)
    pair_macs(2, 2, 2)
    pair_macs(8, 1, 2)
    take(1, 5)
    send_panel(1, 5, 7, 5, at_z)
    share(1, 5)
    take(1, 3)
    share(1, 3)
    take(1, 10)
    take(1, 12)
    pair_macs(3, 2, 2)
    pair_macs(10, 2, 2)
    take(1, 11)
    take(1, 13)
    pair_macs(11, 2, 2)
    take(1, 6)
    share(1, 6)
    take(1, 7)
    share(1, 7)
    pair_macs(6, 1, 2)
    take(1, 14)
    take(1, 15)
    pair_macs(14, 1, 2)

    my_rows = pl.ds(pl.multiple_of(y * slab, slab), slab)
    their_rows = pl.ds(pl.multiple_of((1 - y) * slab, slab), slab)
    for row in (1, 0):
        pure[row] = (3.0 * panels[1, row].astype(jnp.float32) - 2.0 * masked_total(row)).astype(pure.dtype)
        if row == 1:
            go(remote(pure.at[1, my_rows], final.at[1], end_send.at[1], end_recv.at[1], at_far))
            go(remote(pure.at[1, their_rows], final.at[2], end_send.at[2], end_recv.at[2], at_far_y))
    go(remote(pure.at[0, their_rows], final.at[0], end_send.at[0], end_recv.at[0], at_y))

    def place(value, which, side):
        for u in range(slots):
            out[2 * u + which, :, side] = value[:, u * slab : (u + 1) * slab]

    place(pure[0, my_rows], parity, here)
    for number, which, side in ((0, parity, there), (1, 1 - parity, here), (2, 1 - parity, there)):
        ref = final.at[number]
        remote(ref, ref, end_send.at[number], end_recv.at[number], at_y).wait_recv()
        place(final[number], which, side)
    for copy in sent:
        copy.wait_send()


def on_grid(blocks, columns):
    _, band_width, block_size, _ = blocks.shape
    rows = lax.axis_size("rows")
    slots, slab = band_width // 2, block_size // 2
    width = slots * slab
    rank = lax.axis_index("rows")
    live = live_table(columns)
    live_own = lax.dynamic_slice_in_dim(live, rank, 1, 0)[0]
    live_far = lax.dynamic_slice_in_dim(live, lax.rem(rank + rows // 2, rows), 1, 0)[0]
    parity = (rank // 8 + rank % 2) % 2
    by_parity = jnp.stack([live_own, live_far]).reshape(2, slots, 2)
    lane_live = jnp.where(parity == 0, by_parity[:, :, 0], by_parity[:, :, 1])
    lane_live = jnp.repeat(lane_live.astype(jnp.float32), slab, axis=1)
    masked = jnp.where(live_own[:, None, None], blocks[0], jnp.zeros_like(blocks[0]))
    own = masked.reshape(slots, 2, block_size, block_size).transpose(1, 0, 2, 3)
    vmem = pl.BlockSpec(memory_space=pltpu.VMEM)
    dma = pltpu.SemaphoreType.DMA
    result = pl.pallas_call(
        grid_kernel,
        out_shape=jax.ShapeDtypeStruct((band_width, slab, block_size), blocks.dtype),
        in_specs=[vmem, vmem],
        out_specs=vmem,
        scratch_shapes=[
            pltpu.VMEM((2, slots, block_size, block_size), blocks.dtype),
            pltpu.VMEM((2, rows, block_size, width), blocks.dtype),
            pltpu.VMEM((2, block_size, 2 * width), jnp.float32),
            pltpu.VMEM((2, block_size, width), blocks.dtype),
            pltpu.VMEM((3, slab, width), blocks.dtype),
            dma((5,)), dma((5,)), dma((5,)), dma((5,)),
            dma((2, 16)), dma((2, 16)), dma((3,)), dma((3,)),
        ],
        compiler_params=pltpu.CompilerParams(
            collective_id=0, has_side_effects=True, vmem_limit_bytes=60 * 1024 * 1024
        ),
    )(own, lane_live)
    return result[None].astype(jnp.float32)


def from_behind(value, axis, steps):
    count = lax.axis_size(axis)
    pairs = [(source, (source + steps) % count) for source in range(count)]
    return lax.ppermute(value, axis, pairs)


def live_table(columns):
    nrows, band_width = columns.shape
    half_band = band_width // 2
    row_ids = jnp.arange(nrows, dtype=jnp.int32)
    target = (
        row_ids[:, None] + jnp.arange(band_width, dtype=jnp.int32)[None, :] - half_band
    ) % nrows
    return jnp.any(columns[:, None, :] == target[:, :, None], axis=2)


def slot_shift(piece, delta):
    band_width = piece.shape[1]
    if delta >= 0:
        return jnp.concatenate([piece[:, delta:], jnp.zeros_like(piece[:, :delta])], axis=1)
    return jnp.concatenate(
        [jnp.zeros_like(piece[:, :-delta]), piece[:, : band_width + delta]], axis=1
    )


def fetch_band(row_slab, below, above, block_rows, second):
    band_width = row_slab.shape[1]
    pieces = []
    for offset in range(-below, above + 1):
        if offset == 0:
            pieces.append(row_slab)
            continue
        trimmed = (abs(offset) - 1) * block_rows + 1
        if offset > 0:
            outgoing = row_slab[:, : band_width - trimmed]
        else:
            outgoing = row_slab[:, trimmed:]
        if second:
            incoming = from_behind(outgoing, "rows", -offset)
        else:
            incoming = from_behind(outgoing, "rows", -offset)
        filler = jnp.zeros_like(row_slab[:, :trimmed])
        if offset > 0:
            pieces.append(jnp.concatenate([incoming, filler], axis=1))
        else:
            pieces.append(jnp.concatenate([filler, incoming], axis=1))
    return jnp.concatenate(pieces, axis=0)


def merge_groups(totals):
    rounded = lax.optimization_barrier(totals.astype(jnp.bfloat16))
    return jnp.sum(rounded.astype(jnp.float32), axis=0)


def dense_terms(left, window, window_base, groups):
    block_rows, band_width, block_size, inner_width = left.shape
    out_width = window.shape[3]
    half_band = band_width // 2
    group_width = inner_width // groups
    stacked = jnp.stack(
        [
            slot_shift(
                window[window_base + offset : window_base + offset + block_rows], half_band - offset
            )
            for offset in range(band_width)
        ],
        axis=1,
    )
    left_groups = left.reshape(block_rows, band_width, block_size, groups, group_width)
    right_groups = stacked.reshape(
        block_rows, band_width, band_width, groups, group_width, out_width
    )
    totals = jnp.einsum(
        "ramcq,rascqn->crsmn", left_groups, right_groups, preferred_element_type=jnp.float32
    )
    return merge_groups(totals)


def band_terms(left, window, window_base, groups):
    return dense_terms(left, window, window_base, groups)


def per_device(blocks, columns):
    block_rows, band_width, block_size, _ = blocks.shape
    half_band = band_width // 2
    inner_count = lax.axis_size("inner")
    slab_width = block_size // inner_count
    inner_index = lax.axis_index("inner")
    row_owner = lax.axis_index("rows")
    live_own = lax.dynamic_slice_in_dim(live_table(columns), row_owner * block_rows, block_rows, 0)
    live_slots = live_own[:, :, None, None]
    masked = jnp.where(live_slots, blocks, jnp.zeros_like(blocks))
    below = -(-half_band // block_rows)
    above = -(-(half_band - 1) // block_rows)
    window_base = below * block_rows - half_band
    row_slab = lax.dynamic_slice_in_dim(masked, inner_index * slab_width, slab_width, 3)
    window = fetch_band(row_slab, below, above, block_rows, False)
    square = band_terms(masked, window, window_base, inner_count)
    square = jnp.where(live_slots, square, jnp.float32(0.0)).astype(jnp.bfloat16)
    second_window = fetch_band(square, below, above, block_rows, True)
    cubed = band_terms(masked, second_window, window_base, inner_count)
    cubed = jnp.where(live_slots, cubed, jnp.float32(0.0))
    column_slabs = 3.0 * square.astype(jnp.float32) - 2.0 * cubed
    return lax.all_to_all(
        column_slabs.astype(jnp.bfloat16), "inner", split_axis=2, concat_axis=3, tiled=True
    ).astype(column_slabs.dtype)


def solution(mesh):
    in_specs = (P("rows", None, None, None), P())
    out_specs = P("rows", None, "inner", None)

    def step(blocks, columns):
        plain = mesh.shape["rows"] == 16 and mesh.shape["inner"] == 2
        if plain and blocks.shape[:2] == (16, 16) and blocks.shape[2] % 256 == 0:
            chosen = on_grid
        else:
            chosen = per_device
        return jax.shard_map(chosen, mesh=mesh, in_specs=in_specs, out_specs=out_specs, check_vma=False)(
            blocks, columns
        )

    return step
```

```python
import functools

import jax
import jax.numpy as jnp
from jax import lax
from jax.experimental import pallas as pl
from jax.experimental.pallas import tpu as pltpu
from jax.sharding import PartitionSpec as P

MESH = pl.DeviceIdType.MESH

def grid_kernel(columns, raw, out, own, other, lane_live, panels, acc, pure, final, load_sem,
                left_send, left_recv, pass_send, pass_recv, panel_send, panel_recv, end_send, end_recv):
    residues, depth, block, _ = own.shape
    band = residues * depth
    slab = block // 2
    width = depth * slab
    rank, y = lax.axis_index("rows"), lax.axis_index("inner")
    rows = lax.axis_size("rows")
    core, x, z = rank % 2, (rank // 2) % 2, rank // 4
    upper, low = z // 2, z % 2
    to_core, to_x, to_z = 1 - 2 * core, 1 - 2 * x, 1 - 2 * low
    far_rank = lax.rem(rank + rows // 2, rows)
    at_far = {"rows": far_rank, "inner": y}
    at_y = {"rows": rank, "inner": 1 - y}
    at_far_y = {"rows": far_rank, "inner": 1 - y}
    at_z = {"rows": rank + 4 * to_z, "inner": y}
    at_x = {"rows": rank + 2 * to_x, "inner": y}
    at_core = {"rows": rank + to_core, "inner": y}
    everyone = (at_far, at_y, at_far_y, at_z, at_x, at_core)

    barrier = pltpu.get_barrier_semaphore()
    for device in everyone:
        pl.semaphore_signal(barrier, inc=1, device_id=device, device_id_type=MESH)

    here = pl.ds(pl.multiple_of(y * slab, slab), slab)
    there = pl.ds(pl.multiple_of((1 - y) * slab, slab), slab)
    loads = [pltpu.make_async_copy(raw.at[:, which], own.at[which], load_sem.at[which]) for which in range(residues)]
    for load in loads:
        load.start()
    sent = []
    classes = (0, 1)

    def residue(side, q, x_at, core_at):
        return (side + 2 * q + 2 * residues - 2 * x_at - core_at) % residues

    mine = [residue(upper, q, x, core) for q in classes]
    fars = [residue(1 - upper, q, x, core) for q in classes]

    def is_live(row_at, slot):
        target = (row_at + slot + rows - band // 2) % rows
        found = columns[row_at, 0] == target
        for at in range(1, columns.shape[1]):
            found = found | (columns[row_at, at] == target)
        return jnp.where(found, 1, 0)

    def remote(source, target, send_sem, recv_sem, device):
        return pltpu.make_async_remote_copy(
            src_ref=source, dst_ref=target, send_sem=send_sem, recv_sem=recv_sem, device_id=device, device_id_type=MESH
        )

    def go(copy):
        copy.start()
        sent.append(copy)

    def send_left(number):
        which = (fars + mine)[number]
        go(remote(own.at[which, :, :, here], other.at[which, :, :, here],
                  left_send.at[number], left_recv.at[number], at_far))

    def pass_left(number):
        ref = other.at[(mine + fars)[number], :, :, here]
        remote(ref, ref, left_send.at[number], left_recv.at[number], at_far).wait_recv()
        go(remote(ref, ref, pass_send.at[number], pass_recv.at[number], at_y))

    def end_left(number):
        ref = other.at[(mine + fars)[number], :, :, there]
        remote(ref, ref, pass_send.at[number], pass_recv.at[number], at_y).wait_recv()

    def send_panel(product, q, source, target, send_at, device):
        go(remote(panels.at[product, q, source], panels.at[product, q, target],
                  panel_send.at[product, q, send_at], panel_recv.at[product, q, target], device))

    def share(product, q, source):
        send_panel(product, q, source, 8 + source, 8 + source, at_core)

    def take(product, q, source):
        ref = panels.at[product, q, source]
        remote(ref, ref, panel_send.at[product, q, 0], panel_recv.at[product, q, source], at_core).wait_recv()
        if source < 8:
            share(product, q, source)

    def spread(product, q, row):
        send_panel(product, q, row, 2 + row, row, at_z)
        send_panel(product, q, row, 4 + row, 2 + row, at_x)
        share(product, q, row)

    def mac(product, q, source, row, left):
        chip_core, chip, far = source // 8, (source // 2) % 4, source % 2
        delta = 4 * (to_z * (chip % 2) + 2 * far - 2 * row) + 2 * to_x * (chip // 2) + to_core * chip_core
        slot = (delta + band // 2 + 2 * rows) % rows
        theirs = residue(upper, q, x + to_x * (chip // 2), core + to_core * chip_core)
        shift = (theirs - mine[q] + slot) // residues
        block_left = left[slot % residues, slot // residues]
        tile = 2 * slab
        for part in range(width // tile):
            lanes = pl.ds(pl.multiple_of(shift * slab + part * tile, slab), tile)
            acc[row, q, :, lanes] += jnp.dot(
                block_left, panels[product, q, source, :, part * tile : (part + 1) * tile],
                preferred_element_type=jnp.float32,
            )

    middle = slice(depth // 2 * slab, depth // 2 * slab + width)

    def masked_total(row, q):
        keep = lane_live[row : row + 1, q * width : (q + 1) * width] > 0
        return jnp.where(keep, acc[row, q, :, middle], 0.0)

    acc[...] = jnp.zeros_like(acc)
    for row, row_at in enumerate((rank, far_rank)):
        for q in classes:
            for w in range(depth):
                first = q * width + w * slab
                live = is_live(row_at, residues * w + mine[q])
                lane_live[row : row + 1, first : first + slab] = jnp.full((1, slab), live)

    def mask_slot(slot, carry):
        which, w = slot % residues, slot // residues
        keep = jnp.full((1, block), is_live(rank, slot)) > 0
        value = own[which, w]
        own[which, w] = jnp.where(keep, value, jnp.zeros_like(value))
        return carry

    def fill(q, row, left):
        for w in range(depth):
            panels[0, q, row, :, w * slab : (w + 1) * slab] = left[mine[q], w, :, here]

    for load in loads:
        load.wait()
    lax.fori_loop(0, band, mask_slot, 0)
    for q in classes:
        fill(q, 0, own)
    pl.semaphore_wait(barrier, len(everyone))

    for q in classes:
        spread(0, q, 0)
        send_left(q)

    def own_macs(q, first, gap, count):
        def body(n, carry):
            mac(0, q, first + gap * n, 0, own)
            return carry

        lax.fori_loop(0, count, body, 0)

    def both_own_macs(first, gap, count):
        def body(n, carry):
            for q in classes:
                mac(0, q, first + gap * n, 0, own)
            return carry

        lax.fori_loop(0, count, body, 0)

    both_own_macs(0, 1, 1)
    for q in classes:
        take(0, q, 2)
        send_panel(0, q, 2, 6, 4, at_x)
        take(0, q, 4)
        pass_left(q)
        fill(q, 1, other)
        spread(0, q, 1)
    send_left(2)
    send_left(3)
    for q in classes:
        for source in (8, 9, 10, 12):
            take(0, q, source)
    both_own_macs(1, 1, 2)
    both_own_macs(8, 1, 3)
    take(0, 0, 6)
    for q in classes:
        take(0, q, 3)
        send_panel(0, q, 3, 7, 5, at_x)
        take(0, q, 5)
    take(0, 1, 6)
    both_own_macs(3, 1, 4)
    for q in classes:
        for source in (11, 13, 14):
            take(0, q, source)
    both_own_macs(11, 1, 4)
    pass_left(2)
    pass_left(3)

    def second_row(q):
        def body(source, carry):
            mac(0, q, source, 1, other)
            return carry

        lax.fori_loop(0, rows, body, 0)

    def square(row, q):
        panels[1, q, row] = masked_total(row, q).astype(panels.dtype)
        acc[row, q] = jnp.zeros_like(acc[row, q])

    def last_own(q):
        take(0, q, 7)
        take(0, q, 15)
        own_macs(q, 7, 8, 2)
        square(0, q)

    def pair_macs(q, first, gap, count):
        def body(n, carry):
            mac(1, q, first + gap * n, 0, own)
            mac(1, q, first + gap * n, 1, other)
            return carry

        lax.fori_loop(0, count, body, 0)

    last_own(0)
    spread(1, 0, 0)
    for number in range(residues):
        end_left(number)
    second_row(0)
    square(1, 0)
    spread(1, 0, 1)
    last_own(1)
    take(1, 0, 2)
    send_panel(1, 0, 2, 6, 4, at_x)
    spread(1, 1, 0)
    second_row(1)
    square(1, 1)
    take(1, 0, 4)
    take(1, 0, 8)
    take(1, 0, 9)
    take(1, 0, 5)
    send_panel(1, 0, 5, 7, 5, at_z)
    spread(1, 1, 1)

    def finish(q):
        for row in (1, 0):
            total = 3.0 * panels[1, q, row].astype(jnp.float32) - 2.0 * masked_total(row, q)
            pure[row, q] = total.astype(pure.dtype)
            if row == 1:
                go(remote(pure.at[1, q, here], final.at[1, q], end_send.at[1, q], end_recv.at[1, q], at_far))
                go(remote(pure.at[1, q, there], final.at[2, q], end_send.at[2, q], end_recv.at[2, q], at_far_y))
        go(remote(pure.at[0, q, there], final.at[0, q], end_send.at[0, q], end_recv.at[0, q], at_y))

    pair_macs(0, 0, 1, 2)
    pair_macs(0, 8, 1, 2)
    pair_macs(0, 2, 2, 2)
    take(1, 0, 3)
    take(1, 0, 10)
    take(1, 0, 12)
    pair_macs(0, 3, 2, 2)
    pair_macs(0, 10, 2, 2)
    take(1, 1, 2)
    send_panel(1, 1, 2, 6, 4, at_x)
    take(1, 0, 6)
    take(1, 0, 7)
    pair_macs(0, 6, 1, 2)
    for source in (11, 13, 14, 15):
        take(1, 0, source)
    pair_macs(0, 11, 2, 2)
    pair_macs(0, 14, 1, 2)
    finish(0)
    take(1, 1, 4)
    take(1, 1, 5)
    send_panel(1, 1, 5, 7, 5, at_z)
    take(1, 1, 3)
    for source in (8, 9, 10, 12):
        take(1, 1, source)
    pair_macs(1, 0, 1, 6)
    pair_macs(1, 8, 1, 3)
    take(1, 1, 11)
    take(1, 1, 13)
    pair_macs(1, 11, 1, 3)
    for source in (6, 7, 14, 15):
        take(1, 1, source)
    pair_macs(1, 6, 1, 2)
    pair_macs(1, 14, 1, 2)
    finish(1)

    def place(value, which, side):
        for w in range(depth):
            out[residues * w + which, :, side] = value[:, w * slab : (w + 1) * slab]

    for q in classes:
        place(pure[0, q, here], mine[q], here)
    for q in classes:
        for number, which, side in ((0, mine[q], there), (1, fars[q], here), (2, fars[q], there)):
            ref = final.at[number, q]
            remote(ref, ref, end_send.at[number, q], end_recv.at[number, q], at_y).wait_recv()
            place(final[number, q], which, side)
    for copy in sent:
        copy.wait_send()


def on_grid(blocks, columns):
    _, band_width, block_size, _ = blocks.shape
    rows = lax.axis_size("rows")
    residues = 4
    depth, slab = band_width // residues, block_size // 2
    width = depth * slab
    raw = blocks.reshape(depth, residues, block_size, block_size)
    vmem = pl.BlockSpec(memory_space=pltpu.VMEM)
    dma = pltpu.SemaphoreType.DMA
    result = pl.pallas_call(
        grid_kernel,
        out_shape=jax.ShapeDtypeStruct((band_width, slab, block_size), blocks.dtype),
        in_specs=[pl.BlockSpec(memory_space=pltpu.SMEM), pl.BlockSpec(memory_space=pl.ANY)],
        out_specs=vmem,
        scratch_shapes=[
            pltpu.VMEM((residues, depth, block_size, block_size), blocks.dtype),
            pltpu.VMEM((residues, depth, block_size, block_size), blocks.dtype),
            pltpu.VMEM((2, 2 * width), jnp.int32),
            pltpu.VMEM((2, 2, rows, block_size, width), blocks.dtype),
            pltpu.VMEM((2, 2, block_size, 2 * width), jnp.float32),
            pltpu.VMEM((2, 2, block_size, width), blocks.dtype),
            pltpu.VMEM((3, 2, slab, width), blocks.dtype),
            dma((4,)), dma((4,)), dma((4,)), dma((4,)), dma((4,)),
            dma((2, 2, 16)), dma((2, 2, 16)), dma((3, 2)), dma((3, 2)),
        ],
        compiler_params=pltpu.CompilerParams(
            collective_id=0, has_side_effects=True, vmem_limit_bytes=60 * 1024 * 1024
        ),
    )(columns, raw)
    return result[None].astype(jnp.float32)


def from_behind(value, axis, steps):
    count = lax.axis_size(axis)
    pairs = [(source, (source + steps) % count) for source in range(count)]
    return lax.ppermute(value, axis, pairs)


def live_table(columns):
    nrows, band_width = columns.shape
    half_band = band_width // 2
    row_ids = jnp.arange(nrows, dtype=jnp.int32)
    target = (
        row_ids[:, None] + jnp.arange(band_width, dtype=jnp.int32)[None, :] - half_band
    ) % nrows
    return jnp.any(columns[:, None, :] == target[:, :, None], axis=2)


def slot_shift(piece, delta):
    band_width = piece.shape[1]
    if delta >= 0:
        return jnp.concatenate([piece[:, delta:], jnp.zeros_like(piece[:, :delta])], axis=1)
    return jnp.concatenate(
        [jnp.zeros_like(piece[:, :-delta]), piece[:, : band_width + delta]], axis=1
    )


def fetch_band(row_slab, below, above, block_rows, second):
    band_width = row_slab.shape[1]
    pieces = []
    for offset in range(-below, above + 1):
        if offset == 0:
            pieces.append(row_slab)
            continue
        trimmed = (abs(offset) - 1) * block_rows + 1
        if offset > 0:
            outgoing = row_slab[:, : band_width - trimmed]
        else:
            outgoing = row_slab[:, trimmed:]
        if second:
            incoming = from_behind(outgoing, "rows", -offset)
        else:
            incoming = from_behind(outgoing, "rows", -offset)
        filler = jnp.zeros_like(row_slab[:, :trimmed])
        if offset > 0:
            pieces.append(jnp.concatenate([incoming, filler], axis=1))
        else:
            pieces.append(jnp.concatenate([filler, incoming], axis=1))
    return jnp.concatenate(pieces, axis=0)


def merge_groups(totals):
    rounded = lax.optimization_barrier(totals.astype(jnp.bfloat16))
    return jnp.sum(rounded.astype(jnp.float32), axis=0)


def dense_terms(left, window, window_base, groups):
    block_rows, band_width, block_size, inner_width = left.shape
    out_width = window.shape[3]
    half_band = band_width // 2
    group_width = inner_width // groups
    stacked = jnp.stack(
        [
            slot_shift(
                window[window_base + offset : window_base + offset + block_rows], half_band - offset
            )
            for offset in range(band_width)
        ],
        axis=1,
    )
    left_groups = left.reshape(block_rows, band_width, block_size, groups, group_width)
    right_groups = stacked.reshape(
        block_rows, band_width, band_width, groups, group_width, out_width
    )
    totals = jnp.einsum(
        "ramcq,rascqn->crsmn", left_groups, right_groups, preferred_element_type=jnp.float32
    )
    return merge_groups(totals)


def band_terms(left, window, window_base, groups):
    return dense_terms(left, window, window_base, groups)


def per_device(blocks, columns):
    block_rows, band_width, block_size, _ = blocks.shape
    half_band = band_width // 2
    inner_count = lax.axis_size("inner")
    slab_width = block_size // inner_count
    inner_index = lax.axis_index("inner")
    row_owner = lax.axis_index("rows")
    live_own = lax.dynamic_slice_in_dim(live_table(columns), row_owner * block_rows, block_rows, 0)
    live_slots = live_own[:, :, None, None]
    masked = jnp.where(live_slots, blocks, jnp.zeros_like(blocks))
    below = -(-half_band // block_rows)
    above = -(-(half_band - 1) // block_rows)
    window_base = below * block_rows - half_band
    row_slab = lax.dynamic_slice_in_dim(masked, inner_index * slab_width, slab_width, 3)
    window = fetch_band(row_slab, below, above, block_rows, False)
    square = band_terms(masked, window, window_base, inner_count)
    square = jnp.where(live_slots, square, jnp.float32(0.0)).astype(jnp.bfloat16)
    second_window = fetch_band(square, below, above, block_rows, True)
    cubed = band_terms(masked, second_window, window_base, inner_count)
    cubed = jnp.where(live_slots, cubed, jnp.float32(0.0))
    column_slabs = 3.0 * square.astype(jnp.float32) - 2.0 * cubed
    return lax.all_to_all(
        column_slabs.astype(jnp.bfloat16), "inner", split_axis=2, concat_axis=3, tiled=True
    ).astype(column_slabs.dtype)


def solution(mesh):
    in_specs = (P("rows", None, None, None), P())
    out_specs = P("rows", None, "inner", None)

    def step(blocks, columns):
        plain = mesh.shape["rows"] == 16 and mesh.shape["inner"] == 2
        if plain and blocks.shape[:2] == (16, 16) and blocks.shape[2] % 256 == 0:
            chosen = on_grid
        else:
            chosen = per_device
        return jax.shard_map(chosen, mesh=mesh, in_specs=in_specs, out_specs=out_specs, check_vma=False)(
            blocks, columns
        )

    return step
```

```python
import functools

import jax
import jax.numpy as jnp
from jax import lax
from jax.experimental import pallas as pl
from jax.experimental.pallas import tpu as pltpu
from jax.sharding import PartitionSpec as P

MESH = pl.DeviceIdType.MESH

def grid_kernel(columns, raw, out, own, other, lane_live, panels, acc, pure, final, load_sem,
                left_send, left_recv, pass_send, pass_recv, panel_send, panel_recv, end_send, end_recv):
    residues, depth, block, _ = own.shape
    band = residues * depth
    slab = block // 2
    width = depth * slab
    rank, y = lax.axis_index("rows"), lax.axis_index("inner")
    rows = lax.axis_size("rows")
    core, x, z = rank % 2, (rank // 2) % 2, rank // 4
    upper, low = z // 2, z % 2
    to_core, to_x, to_z = 1 - 2 * core, 1 - 2 * x, 1 - 2 * low
    far_rank = lax.rem(rank + rows // 2, rows)
    at_far = {"rows": far_rank, "inner": y}
    at_y = {"rows": rank, "inner": 1 - y}
    at_far_y = {"rows": far_rank, "inner": 1 - y}
    at_z = {"rows": rank + 4 * to_z, "inner": y}
    at_x = {"rows": rank + 2 * to_x, "inner": y}
    at_core = {"rows": rank + to_core, "inner": y}
    everyone = (at_far, at_y, at_far_y, at_z, at_x, at_core)

    barrier = pltpu.get_barrier_semaphore()
    for device in everyone:
        pl.semaphore_signal(barrier, inc=1, device_id=device, device_id_type=MESH)

    here = pl.ds(pl.multiple_of(y * slab, slab), slab)
    there = pl.ds(pl.multiple_of((1 - y) * slab, slab), slab)
    loads = [pltpu.make_async_copy(raw.at[:, which], own.at[which], load_sem.at[which]) for which in range(residues)]
    for load in loads:
        load.start()
    sent = []
    classes = (0, 1)

    def residue(side, q, x_at, core_at):
        return (side + 2 * q + 2 * residues - 2 * x_at - core_at) % residues

    mine = [residue(upper, q, x, core) for q in classes]
    fars = [residue(1 - upper, q, x, core) for q in classes]

    def is_live(row_at, slot):
        target = (row_at + slot + rows - band // 2) % rows
        found = columns[row_at, 0] == target
        for at in range(1, columns.shape[1]):
            found = found | (columns[row_at, at] == target)
        return jnp.where(found, 1, 0)

    def remote(source, target, send_sem, recv_sem, device):
        return pltpu.make_async_remote_copy(
            src_ref=source, dst_ref=target, send_sem=send_sem, recv_sem=recv_sem, device_id=device, device_id_type=MESH
        )

    def go(copy):
        copy.start()
        sent.append(copy)

    def send_left(number):
        which = (fars + mine)[number]
        go(remote(own.at[which, :, :, here], other.at[which, :, :, here],
                  left_send.at[number], left_recv.at[number], at_far))

    def pass_left(number):
        ref = other.at[(mine + fars)[number], :, :, here]
        remote(ref, ref, left_send.at[number], left_recv.at[number], at_far).wait_recv()
        go(remote(ref, ref, pass_send.at[number], pass_recv.at[number], at_y))

    def end_left(number):
        ref = other.at[(mine + fars)[number], :, :, there]
        remote(ref, ref, pass_send.at[number], pass_recv.at[number], at_y).wait_recv()

    def send_panel(product, q, source, target, send_at, device):
        go(remote(panels.at[product, q, source], panels.at[product, q, target],
                  panel_send.at[product, q, send_at], panel_recv.at[product, q, target], device))

    def share(product, q, source):
        send_panel(product, q, source, 8 + source, 8 + source, at_core)

    def take(product, q, source):
        ref = panels.at[product, q, source]
        remote(ref, ref, panel_send.at[product, q, 0], panel_recv.at[product, q, source], at_core).wait_recv()
        if source < 8:
            share(product, q, source)

    def spread(product, q, row):
        send_panel(product, q, row, 2 + row, row, at_z)
        send_panel(product, q, row, 4 + row, 2 + row, at_x)
        share(product, q, row)

    def mac(product, q, source, row, left):
        chip_core, chip, far = source // 8, (source // 2) % 4, source % 2
        delta = 4 * (to_z * (chip % 2) + 2 * far - 2 * row) + 2 * to_x * (chip // 2) + to_core * chip_core
        slot = (delta + band // 2 + 2 * rows) % rows
        theirs = residue(upper, q, x + to_x * (chip // 2), core + to_core * chip_core)
        shift = (theirs - mine[q] + slot) // residues
        block_left = left[slot % residues, slot // residues]
        tile = 2 * slab
        for part in range(width // tile):
            lanes = pl.ds(pl.multiple_of(shift * slab + part * tile, slab), tile)
            acc[row, q, :, lanes] += jnp.dot(
                block_left, panels[product, q, source, :, part * tile : (part + 1) * tile],
                preferred_element_type=jnp.float32,
            )

    middle = slice(depth // 2 * slab, depth // 2 * slab + width)

    def masked_total(row, q):
        keep = lane_live[row : row + 1, q * width : (q + 1) * width] > 0
        return jnp.where(keep, acc[row, q, :, middle], 0.0)

    acc[...] = jnp.zeros_like(acc)
    for row, row_at in enumerate((rank, far_rank)):
        for q in classes:
            for w in range(depth):
                first = q * width + w * slab
                live = is_live(row_at, residues * w + mine[q])
                lane_live[row : row + 1, first : first + slab] = jnp.full((1, slab), live)

    def mask_slot(slot, carry):
        which, w = slot % residues, slot // residues
        keep = jnp.full((1, block), is_live(rank, slot)) > 0
        value = own[which, w]
        own[which, w] = jnp.where(keep, value, jnp.zeros_like(value))
        return carry

    def fill(q, row, left):
        for w in range(depth):
            panels[0, q, row, :, w * slab : (w + 1) * slab] = left[mine[q], w, :, here]

    for load in loads:
        load.wait()
    lax.fori_loop(0, band, mask_slot, 0)
    for q in classes:
        fill(q, 0, own)
    pl.semaphore_wait(barrier, len(everyone))

    for q in classes:
        send_left(q)
        spread(0, q, 0)

    def own_macs(q, first, gap, count):
        def body(n, carry):
            mac(0, q, first + gap * n, 0, own)
            return carry

        lax.fori_loop(0, count, body, 0)

    def both_own_macs(first, gap, count):
        def body(n, carry):
            for q in classes:
                mac(0, q, first + gap * n, 0, own)
            return carry

        lax.fori_loop(0, count, body, 0)

    both_own_macs(0, 1, 1)
    for q in classes:
        take(0, q, 2)
        send_panel(0, q, 2, 6, 4, at_x)
        take(0, q, 4)
        pass_left(q)
        fill(q, 1, other)
        spread(0, q, 1)
    send_left(2)
    send_left(3)
    for q in classes:
        for source in (8, 9, 10, 12):
            take(0, q, source)
    both_own_macs(1, 1, 2)
    both_own_macs(8, 1, 3)
    take(0, 0, 6)
    for q in classes:
        take(0, q, 3)
        send_panel(0, q, 3, 7, 5, at_x)
        take(0, q, 5)
    take(0, 1, 6)
    both_own_macs(3, 1, 4)
    for q in classes:
        for source in (11, 13, 14):
            take(0, q, source)
    both_own_macs(11, 1, 4)
    pass_left(2)
    pass_left(3)

    def second_row(q):
        def body(source, carry):
            mac(0, q, source, 1, other)
            return carry

        lax.fori_loop(0, rows, body, 0)

    def square(row, q):
        panels[1, q, row] = masked_total(row, q).astype(panels.dtype)
        acc[row, q] = jnp.zeros_like(acc[row, q])

    def last_own(q):
        take(0, q, 7)
        take(0, q, 15)
        own_macs(q, 7, 8, 2)
        square(0, q)

    def pair_macs(q, first, gap, count):
        def body(n, carry):
            mac(1, q, first + gap * n, 0, own)
            mac(1, q, first + gap * n, 1, other)
            return carry

        lax.fori_loop(0, count, body, 0)

    last_own(0)
    spread(1, 0, 0)
    for number in range(residues):
        end_left(number)
    second_row(0)
    square(1, 0)
    spread(1, 0, 1)
    last_own(1)
    take(1, 0, 2)
    send_panel(1, 0, 2, 6, 4, at_x)
    spread(1, 1, 0)
    second_row(1)
    square(1, 1)
    take(1, 0, 4)
    take(1, 0, 8)
    take(1, 0, 9)
    take(1, 0, 5)
    send_panel(1, 0, 5, 7, 5, at_z)
    spread(1, 1, 1)

    def finish(q):
        for row in (1, 0):
            total = 3.0 * panels[1, q, row].astype(jnp.float32) - 2.0 * masked_total(row, q)
            pure[row, q] = total.astype(pure.dtype)
            if row == 1:
                go(remote(pure.at[1, q, here], final.at[1, q], end_send.at[1, q], end_recv.at[1, q], at_far))
                go(remote(pure.at[1, q, there], final.at[2, q], end_send.at[2, q], end_recv.at[2, q], at_far_y))
        go(remote(pure.at[0, q, there], final.at[0, q], end_send.at[0, q], end_recv.at[0, q], at_y))

    pair_macs(0, 0, 1, 2)
    pair_macs(0, 8, 1, 2)
    pair_macs(0, 2, 2, 2)
    take(1, 0, 3)
    take(1, 0, 10)
    take(1, 0, 12)
    pair_macs(0, 3, 2, 2)
    pair_macs(0, 10, 2, 2)
    take(1, 1, 2)
    send_panel(1, 1, 2, 6, 4, at_x)
    take(1, 0, 6)
    take(1, 0, 7)
    pair_macs(0, 6, 1, 2)
    for source in (11, 13, 14, 15):
        take(1, 0, source)
    pair_macs(0, 11, 2, 2)
    pair_macs(0, 14, 1, 2)
    finish(0)
    take(1, 1, 4)
    take(1, 1, 5)
    send_panel(1, 1, 5, 7, 5, at_z)
    take(1, 1, 3)
    for source in (8, 9, 10, 12):
        take(1, 1, source)
    pair_macs(1, 0, 1, 6)
    pair_macs(1, 8, 1, 3)
    take(1, 1, 11)
    take(1, 1, 13)
    pair_macs(1, 11, 1, 3)
    for source in (6, 7, 14, 15):
        take(1, 1, source)
    pair_macs(1, 6, 1, 2)
    pair_macs(1, 14, 1, 2)
    finish(1)

    def place(value, which, side):
        for w in range(depth):
            out[residues * w + which, :, side] = value[:, w * slab : (w + 1) * slab]

    for q in classes:
        place(pure[0, q, here], mine[q], here)
    for q in classes:
        for number, which, side in ((0, mine[q], there), (1, fars[q], here), (2, fars[q], there)):
            ref = final.at[number, q]
            remote(ref, ref, end_send.at[number, q], end_recv.at[number, q], at_y).wait_recv()
            place(final[number, q], which, side)
    for copy in sent:
        copy.wait_send()


def on_grid(blocks, columns):
    _, band_width, block_size, _ = blocks.shape
    rows = lax.axis_size("rows")
    residues = 4
    depth, slab = band_width // residues, block_size // 2
    width = depth * slab
    raw = blocks.reshape(depth, residues, block_size, block_size)
    vmem = pl.BlockSpec(memory_space=pltpu.VMEM)
    dma = pltpu.SemaphoreType.DMA
    result = pl.pallas_call(
        grid_kernel,
        out_shape=jax.ShapeDtypeStruct((band_width, slab, block_size), blocks.dtype),
        in_specs=[pl.BlockSpec(memory_space=pltpu.SMEM), pl.BlockSpec(memory_space=pl.ANY)],
        out_specs=vmem,
        scratch_shapes=[
            pltpu.VMEM((residues, depth, block_size, block_size), blocks.dtype),
            pltpu.VMEM((residues, depth, block_size, block_size), blocks.dtype),
            pltpu.VMEM((2, 2 * width), jnp.int32),
            pltpu.VMEM((2, 2, rows, block_size, width), blocks.dtype),
            pltpu.VMEM((2, 2, block_size, 2 * width), jnp.float32),
            pltpu.VMEM((2, 2, block_size, width), blocks.dtype),
            pltpu.VMEM((3, 2, slab, width), blocks.dtype),
            dma((4,)), dma((4,)), dma((4,)), dma((4,)), dma((4,)),
            dma((2, 2, 16)), dma((2, 2, 16)), dma((3, 2)), dma((3, 2)),
        ],
        compiler_params=pltpu.CompilerParams(
            collective_id=0, has_side_effects=True, vmem_limit_bytes=60 * 1024 * 1024
        ),
    )(columns, raw)
    return result[None].astype(jnp.float32)


def from_behind(value, axis, steps):
    count = lax.axis_size(axis)
    pairs = [(source, (source + steps) % count) for source in range(count)]
    return lax.ppermute(value, axis, pairs)


def live_table(columns):
    nrows, band_width = columns.shape
    half_band = band_width // 2
    row_ids = jnp.arange(nrows, dtype=jnp.int32)
    target = (
        row_ids[:, None] + jnp.arange(band_width, dtype=jnp.int32)[None, :] - half_band
    ) % nrows
    return jnp.any(columns[:, None, :] == target[:, :, None], axis=2)


def slot_shift(piece, delta):
    band_width = piece.shape[1]
    if delta >= 0:
        return jnp.concatenate([piece[:, delta:], jnp.zeros_like(piece[:, :delta])], axis=1)
    return jnp.concatenate(
        [jnp.zeros_like(piece[:, :-delta]), piece[:, : band_width + delta]], axis=1
    )


def fetch_band(row_slab, below, above, block_rows, second):
    band_width = row_slab.shape[1]
    pieces = []
    for offset in range(-below, above + 1):
        if offset == 0:
            pieces.append(row_slab)
            continue
        trimmed = (abs(offset) - 1) * block_rows + 1
        if offset > 0:
            outgoing = row_slab[:, : band_width - trimmed]
        else:
            outgoing = row_slab[:, trimmed:]
        if second:
            incoming = from_behind(outgoing, "rows", -offset)
        else:
            incoming = from_behind(outgoing, "rows", -offset)
        filler = jnp.zeros_like(row_slab[:, :trimmed])
        if offset > 0:
            pieces.append(jnp.concatenate([incoming, filler], axis=1))
        else:
            pieces.append(jnp.concatenate([filler, incoming], axis=1))
    return jnp.concatenate(pieces, axis=0)


def merge_groups(totals):
    rounded = lax.optimization_barrier(totals.astype(jnp.bfloat16))
    return jnp.sum(rounded.astype(jnp.float32), axis=0)


def dense_terms(left, window, window_base, groups):
    block_rows, band_width, block_size, inner_width = left.shape
    out_width = window.shape[3]
    half_band = band_width // 2
    group_width = inner_width // groups
    stacked = jnp.stack(
        [
            slot_shift(
                window[window_base + offset : window_base + offset + block_rows], half_band - offset
            )
            for offset in range(band_width)
        ],
        axis=1,
    )
    left_groups = left.reshape(block_rows, band_width, block_size, groups, group_width)
    right_groups = stacked.reshape(
        block_rows, band_width, band_width, groups, group_width, out_width
    )
    totals = jnp.einsum(
        "ramcq,rascqn->crsmn", left_groups, right_groups, preferred_element_type=jnp.float32
    )
    return merge_groups(totals)


def band_terms(left, window, window_base, groups):
    return dense_terms(left, window, window_base, groups)


def per_device(blocks, columns):
    block_rows, band_width, block_size, _ = blocks.shape
    half_band = band_width // 2
    inner_count = lax.axis_size("inner")
    slab_width = block_size // inner_count
    inner_index = lax.axis_index("inner")
    row_owner = lax.axis_index("rows")
    live_own = lax.dynamic_slice_in_dim(live_table(columns), row_owner * block_rows, block_rows, 0)
    live_slots = live_own[:, :, None, None]
    masked = jnp.where(live_slots, blocks, jnp.zeros_like(blocks))
    below = -(-half_band // block_rows)
    above = -(-(half_band - 1) // block_rows)
    window_base = below * block_rows - half_band
    row_slab = lax.dynamic_slice_in_dim(masked, inner_index * slab_width, slab_width, 3)
    window = fetch_band(row_slab, below, above, block_rows, False)
    square = band_terms(masked, window, window_base, inner_count)
    square = jnp.where(live_slots, square, jnp.float32(0.0)).astype(jnp.bfloat16)
    second_window = fetch_band(square, below, above, block_rows, True)
    cubed = band_terms(masked, second_window, window_base, inner_count)
    cubed = jnp.where(live_slots, cubed, jnp.float32(0.0))
    column_slabs = 3.0 * square.astype(jnp.float32) - 2.0 * cubed
    return lax.all_to_all(
        column_slabs.astype(jnp.bfloat16), "inner", split_axis=2, concat_axis=3, tiled=True
    ).astype(column_slabs.dtype)


def solution(mesh):
    in_specs = (P("rows", None, None, None), P())
    out_specs = P("rows", None, "inner", None)

    def step(blocks, columns):
        plain = mesh.shape["rows"] == 16 and mesh.shape["inner"] == 2
        if plain and blocks.shape[:2] == (16, 16) and blocks.shape[2] % 256 == 0:
            chosen = on_grid
        else:
            chosen = per_device
        return jax.shard_map(chosen, mesh=mesh, in_specs=in_specs, out_specs=out_specs, check_vma=False)(
            blocks, columns
        )

    return step
```
